32 devices in a mesh: section: 2 (over core), dev: 16 (over z, y, x).
Axes of the slice: x: 2, y: 2, z: 4, core: 2. Of those that a mesh axis runs over, the one named last changes fastest.
Arguments:
- indices: int32 [2048, 32, 8], P(('section', 'dev')), may hold values from 0 to 32767
- pool_len: int32 [32], replicated, may hold values from 1 to 8
- tables: bfloat16 [1048576, 128], P(('section', 'dev')), may hold values from -3 to 3
- w_first: bfloat16 [4096, 4096], P('dev', 'section'), may hold values from -0.09375 to 0.09375
- b_first: bfloat16 [4096], P('section'), may hold values from -3 to 3
- w_out: bfloat16 [4096], P('section'), may hold values from -0.09375 to 0.09375
Outputs:
- logits: float32 [2048], P('dev')
The draws below stay inside these ranges and needn't reach their ends.
Inputs may be any that keep to these rules, and one draw needn't show every extreme that they name: `indices`: ids of rows of the table named by the second index.
All inputs are finite; a program needn't handle non-finite values.
Results may differ from the reference program's by a relative error of at most 0.0095.
Values may be sent and summed in bfloat16 or wider, within the bound.
A program may use at most 128 MiB of HBM per device.

```python
import jax
import jax.numpy as jnp
from jax import lax

E = 128
HID = 4096
TABLES = 32
POOL = 8
ROWS_DEV = 32768
RSPLIT = 1
ROWS = 32768
FEAT = 4096
BATCH = 2048


def plant(array, key, low, top_value):
    longest = array.shape.index(max(array.shape))
    spots = []
    for shift in (0, 1):
        where = [jax.random.randint(jax.random.fold_in(key, axis), (), 0, length) for axis, length in enumerate(array.shape)]
        where[longest] = (where[longest] + shift) % array.shape[longest]
        spots.append(tuple(where))
    return array.at[spots[0]].set(low).at[spots[1]].set(top_value)


def block_levels(key, shape, split, smallest, largest):
    level, own = 1.0, jax.random.fold_in(key, 6)
    for position, parts in split:
        draws = jnp.exp(jax.random.uniform(jax.random.fold_in(own, position), (parts,), jnp.float32, smallest / len(split), largest / len(split)))
        level = level * jnp.repeat(draws, shape[position] // parts).reshape([-1 if axis == position else 1 for axis in range(len(shape))])
    return level


def scatter_about(rng, dims, spread, limit, split=(), dtype=jnp.bfloat16):
    factor_of = block_levels(rng, dims, split, -0.22, 0.18) if split else 1.0
    values = jax.random.normal(rng, dims, jnp.float32) * spread * factor_of
    return jnp.minimum(jnp.maximum(values, -limit), limit).astype(dtype)


def setup_inputs(seed: int = 0) -> dict:
    arg_keys = jax.random.split(jax.random.key(seed), 7)
    indices = plant(jax.random.randint(arg_keys[0], (BATCH, TABLES, POOL), 0, ROWS), jax.random.fold_in(arg_keys[0], 1), 0, ROWS - 1).astype(jnp.int32)
    pool_len = plant(jax.random.randint(arg_keys[1], (TABLES,), 1, POOL + 1), jax.random.fold_in(arg_keys[1], 1), 1, POOL).astype(jnp.int32)
    tables = scatter_about(arg_keys[2], (TABLES * ROWS, E), 0.5, 3.0, ((0, 32),))
    w_first = scatter_about(arg_keys[3], (FEAT, HID), FEAT ** -0.5, 0.09375, ((0, 16), (1, 2)))
    b_first = scatter_about(arg_keys[4], (HID,), 0.5, 3.0, ((0, 2),))
    w_out = scatter_about(arg_keys[5], (HID,), HID ** -0.5, 0.09375, ((0, 2),))
    return {"indices": indices, "pool_len": pool_len, "tables": tables, "w_first": w_first, "b_first": b_first, "w_out": w_out}


def pool_table(inputs):
    table_rows, bag_ids, live_count = inputs
    gathered = jnp.take(table_rows, bag_ids, axis=0).astype(jnp.float32)
    slot_live = (jnp.arange(POOL) < live_count).astype(jnp.float32)
    row_block = bag_ids // ROWS_DEV
    owners = (row_block[:, :, None] == jnp.arange(RSPLIT)[None, None, :]).astype(jnp.float32)
    owners = owners * slot_live[None, :, None]
    partial_value = jnp.einsum('bpr,bpe->rbe', owners, gathered).astype(jnp.bfloat16)
    return jnp.sum(partial_value.astype(jnp.float32), axis=0).astype(jnp.bfloat16)


def reference(indices, pool_len, tables, w_first, b_first, w_out):
    table_view = tables.reshape(TABLES, ROWS, E)
    pooled = lax.map(pool_table, (table_view, jnp.transpose(indices, (1, 0, 2)), pool_len))
    flat_feat = jnp.transpose(pooled, (1, 0, 2)).reshape(BATCH, FEAT)
    pre_act = jnp.dot(flat_feat, w_first, preferred_element_type=jnp.float32) + b_first.astype(jnp.float32)
    hidden = jnp.maximum(pre_act, 0.0)
    return jnp.sum(hidden * w_out.astype(jnp.float32)[None, :], axis=1)
```

```python
import functools

import jax
import jax.numpy as jnp
from jax import lax
from jax.experimental import pallas as pl
from jax.experimental.pallas import tpu as pltpu
from jax.sharding import PartitionSpec as P

VMEM_LIMIT = 60 * 1024 * 1024
PLANE = 4


def bag_kernel(table_chunks, bags_per_step, pool_size, table_ref, ids_ref, out_ref, staged, wide, sums, sems):
    rows, _ = table_ref.shape
    chunk = rows // table_chunks

    def fetch(c):
        return pltpu.make_async_copy(table_ref.at[pl.ds(c * chunk, chunk)], staged.at[c % 2], sems.at[c % 2])

    fetch(0).start()
    wide[pl.ds(rows, 8), :] = jnp.zeros((8, wide.shape[1]), jnp.float32)
    for c in range(table_chunks):
        if c + 1 < table_chunks:
            fetch(c + 1).start()
        fetch(c).wait()
        step = 256

        def widen(k, carry):
            at = pl.multiple_of(k * step, step)
            wide[pl.ds(c * chunk + at, step), :] = staged[c % 2, pl.ds(at, step), :].astype(jnp.float32)
            return carry

        lax.fori_loop(0, chunk // step, widen, 0)

    def bags(r, carry):
        for b in range(bags_per_step):
            total = None
            for p in range(pool_size):
                row = wide[pl.ds(ids_ref[r, b * pool_size + p], 1), :]
                total = row if total is None else total + row
            sums[pl.ds(r * bags_per_step + b, 1), :] = total
        return carry

    lax.fori_loop(0, ids_ref.shape[0], bags, 0)
    out_ref[...] = sums[...].astype(jnp.bfloat16)


def pool_bags(table, ids, pool_size):
    rows, emb = table.shape
    bags_per_step = ids.shape[1] // pool_size
    n_bags = ids.shape[0] * bags_per_step
    chunks = 8
    return pl.pallas_call(
        functools.partial(bag_kernel, chunks, bags_per_step, pool_size),
        out_shape=jax.ShapeDtypeStruct((n_bags, emb), jnp.bfloat16),
        in_specs=[pl.BlockSpec(memory_space=pl.ANY), pl.BlockSpec(memory_space=pltpu.SMEM)],
        out_specs=pl.BlockSpec(memory_space=pltpu.VMEM),
        scratch_shapes=[
            pltpu.VMEM((2, rows // chunks, emb), jnp.bfloat16),
            pltpu.VMEM((rows + 8, emb), jnp.float32),
            pltpu.VMEM((n_bags, emb), jnp.float32),
            pltpu.SemaphoreType.DMA((2,)),
        ],
        compiler_params=pltpu.CompilerParams(vmem_limit_bytes=VMEM_LIMIT),
        cost_estimate=pl.CostEstimate(flops=n_bags * pool_size * emb * 600, bytes_accessed=rows * emb * 2, transcendentals=0),
        name="pool_bags",
    )(table, ids)


def dense_kernel(
    secs, devs, pooled_ref, w_ref, b_ref, wo_ref, out_ref,
    feats, pre, outgoing, incoming, mine, theirs,
    fsend, frecv, psend, precv, lsend, lrecv,
):
    emb = pooled_ref.shape[1]
    depth, hid = w_ref.shape
    per_dev = depth // (devs // PLANE)
    tables_dev = per_dev // emb
    planes = devs // PLANE
    group = pooled_ref.shape[0] // planes
    block = group // PLANE
    tiles = psend.shape[1]
    tile = hid // tiles
    sec, dev = lax.axis_index("section"), lax.axis_index("dev")
    me = sec * devs + dev
    plane, inner = dev // PLANE, dev % PLANE

    barrier = pltpu.get_barrier_semaphore()
    for k in range(1, secs * devs):
        other = lax.rem(me + k, secs * devs)
        pl.semaphore_signal(barrier, inc=1, device_id={"section": other // devs, "dev": lax.rem(other, devs)})
    pl.semaphore_wait(barrier, secs * devs - 1)

    owner = me // tables_dev
    slot = owner // PLANE * tables_dev + lax.rem(me, tables_dev)
    column = pl.ds(pl.multiple_of(slot * emb, emb), emb)
    to_inner = lax.rem(owner, PLANE)
    keeps = to_inner == inner
    copies = []
    for k in range(planes):
        for c in range(secs):
            to_plane = lax.rem(plane + k, planes)
            to_sec = lax.rem(sec + c, secs)
            src = pooled_ref.at[pl.ds(pl.multiple_of(to_plane * group, group), group), :]
            dst = feats.at[:, column]
            copy = pltpu.make_async_remote_copy(
                src_ref=src, dst_ref=dst,
                send_sem=fsend.at[k, c], recv_sem=frecv.at[slot],
                device_id={"section": to_sec, "dev": to_plane * PLANE + to_inner},
            )
            if k == 0 and c == 0:
                local = pltpu.make_async_copy(src, dst, frecv.at[slot])

                @pl.when(keeps)
                def _():
                    local.start()

                @pl.when(jnp.logical_not(keeps))
                def _():
                    copy.start()
            else:
                copy.start()
            copies.append(copy)
    for t in range(depth // emb):
        part = feats.at[:, pl.ds(t * emb, emb)]
        pltpu.make_async_copy(part, part, frecv.at[t]).wait()

    partials = []
    for n in range(tiles):
        cols = pl.ds(n * tile, tile)
        got = jnp.dot(feats[...], w_ref[:, cols], preferred_element_type=jnp.float32)
        pre[:, cols] = got
        outgoing[:, cols] = got.astype(jnp.bfloat16)
        for k in range(1, PLANE):
            to = lax.rem(inner + k, PLANE)
            copy = pltpu.make_async_remote_copy(
                src_ref=outgoing.at[pl.ds(pl.multiple_of(to * block, block), block), cols],
                dst_ref=incoming.at[k - 1, :, cols],
                send_sem=psend.at[k - 1, n], recv_sem=precv.at[k - 1, n],
                device_id={"section": sec, "dev": plane * PLANE + to},
            )
            copy.start()
            partials.append(copy)

    acc = jnp.zeros((block, 128), jnp.float32)
    own = pl.ds(pl.multiple_of(inner * block, block), block)
    for n in range(tiles):
        cols = pl.ds(n * tile, tile)
        total = pre[own, cols]
        for k in range(1, PLANE):
            partials[n * (PLANE - 1) + k - 1].wait_recv()
            total = total + incoming[k - 1, :, cols].astype(jnp.float32)
        hidden = jnp.maximum(total + b_ref[:, cols].astype(jnp.float32), 0.0)
        weighed = hidden * wo_ref[:, cols].astype(jnp.float32)
        for q in range(tile // 128):
            acc = acc + weighed[:, q * 128:(q + 1) * 128]
    mine[...] = jnp.sum(acc.T, axis=0, keepdims=True)
    swap = pltpu.make_async_remote_copy(
        src_ref=mine, dst_ref=theirs, send_sem=lsend, recv_sem=lrecv,
        device_id={"section": 1 - sec, "dev": dev},
    )
    swap.start()
    swap.wait()
    out_ref[...] = mine[...] + theirs[...]
    for copy in partials:
        copy.wait_send()
    for n, copy in enumerate(copies):
        if n == 0:
            @pl.when(jnp.logical_not(keeps))
            def _():
                copies[0].wait_send()
        else:
            copy.wait_send()


def dense(secs, devs, pooled, weights, bias, w_out):
    n_bags, emb = pooled.shape
    depth, hid = weights.shape
    planes = devs // PLANE
    group = n_bags // planes
    block = group // PLANE
    tiles = 4
    vm = pl.BlockSpec(memory_space=pltpu.VMEM)
    return pl.pallas_call(
        functools.partial(dense_kernel, secs, devs),
        out_shape=jax.ShapeDtypeStruct((1, block), jnp.float32),
        in_specs=[vm] * 4,
        out_specs=vm,
        scratch_shapes=[
            pltpu.VMEM((group, depth), jnp.bfloat16),
            pltpu.VMEM((group, hid), jnp.float32),
            pltpu.VMEM((group, hid), jnp.bfloat16),
            pltpu.VMEM((PLANE - 1, block, hid), jnp.bfloat16),
            pltpu.VMEM((1, block), jnp.float32),
            pltpu.VMEM((1, block), jnp.float32),
            pltpu.SemaphoreType.DMA((planes, secs)),
            pltpu.SemaphoreType.DMA((depth // emb,)),
            pltpu.SemaphoreType.DMA((PLANE - 1, tiles)),
            pltpu.SemaphoreType.DMA((PLANE - 1, tiles)),
            pltpu.SemaphoreType.DMA,
            pltpu.SemaphoreType.DMA,
        ],
        compiler_params=pltpu.CompilerParams(collective_id=0, has_side_effects=True, vmem_limit_bytes=VMEM_LIMIT),
        name="dense",
    )(pooled, weights, bias, w_out)


def body(indices, pool_len, tables, w_first, b_first, w_out):
    sec_count = lax.axis_size("section")
    dev_count = lax.axis_size("dev")
    devices = sec_count * dev_count
    dev_rows, n_tables, pool_size = indices.shape
    rows_dev, emb_width = tables.shape
    row_split = devices // n_tables
    position = lax.axis_index("section") * dev_count + lax.axis_index("dev")
    table_id = position // row_split
    first_row = position % row_split * rows_dev
    outgoing = jnp.transpose(indices, (1, 0, 2)).reshape(n_tables, dev_rows * pool_size)
    outgoing = jnp.repeat(outgoing, row_split, axis=0)
    arrived = lax.all_to_all(outgoing, ("section", "dev"), split_axis=0, concat_axis=0, tiled=True)
    all_rows = devices * dev_rows
    wanted = arrived.reshape(all_rows * pool_size // 128, 128) - first_row
    live_slots = jnp.sum(jnp.where(jnp.arange(n_tables) == table_id, pool_len, 0))
    slot = jnp.arange(128) % pool_size
    usable = (wanted >= 0) & (wanted < rows_dev) & (slot < live_slots)[None, :]
    safe_rows = jnp.where(usable, wanted, rows_dev)
    partial_value = pool_bags(tables, safe_rows, pool_size)
    planes = dev_count // PLANE
    if row_split == 1 and sec_count == 2 and w_first.shape[0] % emb_width == 0 and dev_count % PLANE == 0:
        columns = [[p * PLANE + i for p in range(planes)] for i in range(PLANE)]
        near_weights = lax.all_gather(w_first, "dev", axis=0, tiled=True, axis_index_groups=columns)
        logits = dense(sec_count, dev_count, partial_value, near_weights, b_first[None, :], w_out[None, :])
        return logits.reshape(logits.shape[1])
    ordered = jnp.transpose(
        partial_value.reshape(dev_count, sec_count, dev_rows, emb_width), (1, 0, 2, 3)
    )
    received = lax.all_to_all(
        ordered.reshape(devices, dev_rows, emb_width),
        ("section", "dev"),
        split_axis=0,
        concat_axis=0,
        tiled=True,
    )
    summed = jnp.sum(
        received.reshape(n_tables, row_split, dev_rows, emb_width).astype(jnp.float32), axis=1
    )
    features = jnp.transpose(summed.astype(jnp.bfloat16), (1, 0, 2)).reshape(
        dev_rows, n_tables * emb_width
    )
    samples = lax.all_gather(features, "section", axis=0, tiled=True)
    whole_weights = lax.all_gather(w_first, "dev", axis=0, tiled=True)
    pre_act = jnp.dot(samples, whole_weights, preferred_element_type=jnp.float32)
    hidden = jnp.maximum(pre_act + b_first.astype(jnp.float32)[None, :], 0.0)
    logit_part = jnp.sum(hidden * w_out.astype(jnp.float32)[None, :], axis=1)
    return lax.psum(logit_part, "section")


def solution(mesh):
    placed = (
        P(("section", "dev"), None, None),
        P(),
        P(("section", "dev"), None),
        P("dev", "section"),
        P("section"),
        P("section"),
    )
    return jax.shard_map(body, mesh=mesh, in_specs=placed, out_specs=P("dev"), check_vma=False)
```

```python
import functools

import jax
import jax.numpy as jnp
from jax import lax
from jax.experimental import pallas as pl
from jax.experimental.pallas import tpu as pltpu
from jax.sharding import PartitionSpec as P

VMEM_LIMIT = 60 * 1024 * 1024
PLANE = 4


def bag_kernel(table_chunks, bags_per_step, pool_size, table_ref, ids_ref, out_ref, staged, wide, sums, sems):
    rows, _ = table_ref.shape
    chunk = rows // table_chunks

    def fetch(c):
        return pltpu.make_async_copy(table_ref.at[pl.ds(c * chunk, chunk)], staged.at[c % 2], sems.at[c % 2])

    fetch(0).start()
    wide[pl.ds(rows, 8), :] = jnp.zeros((8, wide.shape[1]), jnp.float32)
    for c in range(table_chunks):
        if c + 1 < table_chunks:
            fetch(c + 1).start()
        fetch(c).wait()
        step = 256

        def widen(k, carry):
            at = pl.multiple_of(k * step, step)
            wide[pl.ds(c * chunk + at, step), :] = staged[c % 2, pl.ds(at, step), :].astype(jnp.float32)
            return carry

        lax.fori_loop(0, chunk // step, widen, 0)

    def bags(r, carry):
        for b in range(bags_per_step):
            total = None
            for p in range(pool_size):
                row = wide[pl.ds(ids_ref[r, b * pool_size + p], 1), :]
                total = row if total is None else total + row
            sums[pl.ds(r * bags_per_step + b, 1), :] = total
        return carry

    lax.fori_loop(0, ids_ref.shape[0], bags, 0)
    out_ref[...] = sums[...].astype(jnp.bfloat16)


def pool_bags(table, ids, pool_size):
    rows, emb = table.shape
    bags_per_step = ids.shape[1] // pool_size
    n_bags = ids.shape[0] * bags_per_step
    chunks = 8
    return pl.pallas_call(
        functools.partial(bag_kernel, chunks, bags_per_step, pool_size),
        out_shape=jax.ShapeDtypeStruct((n_bags, emb), jnp.bfloat16),
        in_specs=[pl.BlockSpec(memory_space=pl.ANY), pl.BlockSpec(memory_space=pltpu.SMEM)],
        out_specs=pl.BlockSpec(memory_space=pltpu.VMEM),
        scratch_shapes=[
            pltpu.VMEM((2, rows // chunks, emb), jnp.bfloat16),
            pltpu.VMEM((rows + 8, emb), jnp.float32),
            pltpu.VMEM((n_bags, emb), jnp.float32),
            pltpu.SemaphoreType.DMA((2,)),
        ],
        compiler_params=pltpu.CompilerParams(vmem_limit_bytes=VMEM_LIMIT),
        cost_estimate=pl.CostEstimate(flops=n_bags * pool_size * emb * 600, bytes_accessed=rows * emb * 2, transcendentals=0),
        name="pool_bags",
    )(table, ids)


def step_kernel(
    secs, devs, pool_size,
    ids_ref, len_ref, table_ref, w_ref, b_ref, wo_ref, out_ref,
    ids_in, ids_safe, ids_smem, staged, wide, sums, pooled, feats, weights, pre, outgoing, incoming, mine, theirs,
    isend, irecv, icopy, tsem, fsend, frecv, wsend, wrecv, wlocal, psend, precv, lsend, lrecv,
):
    rows, emb = table_ref.shape
    count = secs * devs
    per_dev, hid = w_ref.shape
    depth = PLANE * per_dev
    tables_dev = per_dev // emb
    planes = devs // PLANE
    block = pooled.shape[2]
    tiles = psend.shape[1]
    tile = hid // tiles
    sec, dev = lax.axis_index("section"), lax.axis_index("dev")
    me = sec * devs + dev
    plane, inner = dev // PLANE, lax.rem(dev, PLANE)

    def device(position):
        return {"section": position // devs, "dev": lax.rem(position, devs)}

    chunks = 8
    chunk = rows // chunks

    def fetch(c):
        return pltpu.make_async_copy(table_ref.at[pl.ds(c * chunk, chunk)], staged.at[c % 2], tsem.at[c % 2])

    fetch(0).start()
    own_weights = pltpu.make_async_copy(w_ref, weights.at[inner], wlocal)
    own_weights.start()
    own_ids = pltpu.make_async_copy(ids_ref.at[me], ids_in.at[me], irecv)
    own_ids.start()

    barrier = pltpu.get_barrier_semaphore()
    for k in range(1, count):
        pl.semaphore_signal(barrier, inc=1, device_id=device(lax.rem(me + k, count)))
    pl.semaphore_wait(barrier, count - 1)

    for k in range(1, count):
        other = lax.rem(me + k, count)
        pltpu.make_async_remote_copy(
            src_ref=ids_ref.at[other], dst_ref=ids_in.at[me], send_sem=isend, recv_sem=irecv,
            device_id=device(other),
        ).start()

    shipped = []

    def ship(n):
        cols = pl.ds(n * tile, tile)
        for k in range(1, PLANE):
            copy = pltpu.make_async_remote_copy(
                src_ref=w_ref.at[:, cols], dst_ref=weights.at[inner, :, cols],
                send_sem=wsend.at[k - 1, n], recv_sem=wrecv.at[k - 1, n],
                device_id={"section": sec, "dev": plane * PLANE + lax.rem(inner + k, PLANE)},
            )
            copy.start()
            shipped.append(copy)

    ship(0)
    ship(1)

    wide[pl.ds(rows, 8), :] = jnp.zeros((8, emb), jnp.float32)
    step = 256
    for c in range(chunks):
        if c + 1 < chunks:
            fetch(c + 1).start()
        fetch(c).wait()

        def widen(k, carry):
            at = pl.multiple_of(k * step, step)
            wide[pl.ds(c * chunk + at, step), :] = staged[c % 2, pl.ds(at, step), :].astype(jnp.float32)
            return carry

        lax.fori_loop(0, chunk // step, widen, 0)

    pltpu.make_async_copy(ids_in, ids_in, irecv).wait()
    lane_slot = lax.rem(lax.broadcasted_iota(jnp.int32, ids_in.shape, 2), pool_size)
    ids_safe[...] = jnp.where(lane_slot < len_ref[me], ids_in[...], rows)
    to_smem = pltpu.make_async_copy(ids_safe, ids_smem, icopy)
    to_smem.start()
    to_smem.wait()

    per_row = 128 // pool_size
    id_rows = ids_in.shape[1]
    block_rows = block // per_row
    owner = me // tables_dev
    to_plane = owner // PLANE
    slot = lax.rem(owner, PLANE) * tables_dev + lax.rem(me, tables_dev)
    column = pl.ds(pl.multiple_of(slot * emb, emb), emb)
    keeps = to_plane == plane
    copies = []
    for k in list(range(1, PLANE)) + [0]:
        to_inner = lax.rem(inner + k, PLANE)

        def bags(n, carry):
            at_plane, r = n // block_rows, lax.rem(n, block_rows)
            line = (at_plane * PLANE + to_inner) * block_rows + r
            source, part = line // id_rows, lax.rem(line, id_rows)
            for q in range(per_row):
                total = None
                for p in range(pool_size):
                    row = wide[pl.ds(ids_smem[source, part, q * pool_size + p], 1), :]
                    total = row if total is None else total + row
                sums[at_plane, to_inner, pl.ds(r * per_row + q, 1), :] = total
            return carry

        lax.fori_loop(0, planes * block_rows, bags, 0)
        pooled[:, to_inner] = sums[:, to_inner].astype(jnp.bfloat16)
        for c in range(secs):
            source_part, dst = pooled.at[:, to_inner], feats.at[:, :, column]
            copy = pltpu.make_async_remote_copy(
                src_ref=source_part, dst_ref=dst,
                send_sem=fsend.at[k, c], recv_sem=frecv.at[slot],
                device_id={"section": lax.rem(sec + c, secs), "dev": to_plane * PLANE + to_inner},
            )
            if k == 0 and c == 0:
                local = pltpu.make_async_copy(source_part, dst, frecv.at[slot])

                @pl.when(keeps)
                def _():
                    local.start()

                @pl.when(jnp.logical_not(keeps))
                def _():
                    copy.start()

                kept = copy
            else:
                copy.start()
                copies.append(copy)
        if k == 1:
            ship(2)
        if k == 3:
            ship(3)
    for t in range(depth // emb):
        part = feats.at[:, :, pl.ds(t * emb, emb)]
        pltpu.make_async_copy(part, part, frecv.at[t]).wait()

    own_weights.wait()
    partials = []
    for n in range(tiles):
        cols = pl.ds(n * tile, tile)
        for k in range(1, PLANE):
            shipped[n * (PLANE - 1) + k - 1].wait_recv()
        got = jnp.dot(
            feats[...].reshape(planes * block, depth), weights[:, :, cols].reshape(depth, tile),
            preferred_element_type=jnp.float32,
        ).reshape(planes, block, tile)
        pre[:, :, cols] = got
        outgoing[:, :, cols] = got.astype(jnp.bfloat16)
        for k in range(1, planes):
            to = lax.rem(plane + k, planes)
            copy = pltpu.make_async_remote_copy(
                src_ref=outgoing.at[to, :, cols], dst_ref=incoming.at[k - 1, :, cols],
                send_sem=psend.at[k - 1, n], recv_sem=precv.at[k - 1, n],
                device_id={"section": sec, "dev": to * PLANE + inner},
            )
            copy.start()
            partials.append(copy)

    acc = jnp.zeros((block, 128), jnp.float32)
    for n in range(tiles):
        cols = pl.ds(n * tile, tile)
        total = pre[plane, :, cols]
        for k in range(1, planes):
            partials[n * (planes - 1) + k - 1].wait_recv()
            total = total + incoming[k - 1, :, cols].astype(jnp.float32)
        hidden = jnp.maximum(total + b_ref[:, cols].astype(jnp.float32), 0.0)
        weighed = hidden * wo_ref[:, cols].astype(jnp.float32)
        for q in range(tile // 128):
            acc = acc + weighed[:, q * 128:(q + 1) * 128]
    mine[...] = jnp.sum(acc.T, axis=0, keepdims=True)
    swap = pltpu.make_async_remote_copy(
        src_ref=mine, dst_ref=theirs, send_sem=lsend, recv_sem=lrecv,
        device_id={"section": 1 - sec, "dev": dev},
    )
    swap.start()
    swap.wait()
    out_ref[...] = mine[...] + theirs[...]
    for copy in partials + shipped + copies:
        copy.wait_send()

    @pl.when(jnp.logical_not(keeps))
    def _():
        kept.wait_send()

    sent = ids_in.at[pl.ds(0, count - 1)]
    pltpu.make_async_copy(sent, sent, isend).wait()


def whole_step(secs, devs, pool_size, ids, pool_len, table, w_first, bias, w_out):
    rows, emb = table.shape
    per_dev, hid = w_first.shape
    count = secs * devs
    planes = devs // PLANE
    depth = PLANE * per_dev
    block = ids.shape[1] * 128 // pool_size * secs
    tiles = 4
    vm = pl.BlockSpec(memory_space=pltpu.VMEM)
    anywhere = pl.BlockSpec(memory_space=pl.ANY)
    dma = pltpu.SemaphoreType.DMA
    return pl.pallas_call(
        functools.partial(step_kernel, secs, devs, pool_size),
        out_shape=jax.ShapeDtypeStruct((1, block), jnp.float32),
        in_specs=[vm, pl.BlockSpec(memory_space=pltpu.SMEM), anywhere, anywhere, vm, vm],
        out_specs=vm,
        scratch_shapes=[
            pltpu.VMEM(ids.shape, jnp.int32),
            pltpu.VMEM(ids.shape, jnp.int32),
            pltpu.SMEM(ids.shape, jnp.int32),
            pltpu.VMEM((2, rows // 8, emb), jnp.bfloat16),
            pltpu.VMEM((rows + 8, emb), jnp.float32),
            pltpu.VMEM((planes, PLANE, block, emb), jnp.float32),
            pltpu.VMEM((planes, PLANE, block, emb), jnp.bfloat16),
            pltpu.VMEM((planes, block, depth), jnp.bfloat16),
            pltpu.VMEM((PLANE, per_dev, hid), jnp.bfloat16),
            pltpu.VMEM((planes, block, hid), jnp.float32),
            pltpu.VMEM((planes, block, hid), jnp.bfloat16),
            pltpu.VMEM((planes - 1, block, hid), jnp.bfloat16),
            pltpu.VMEM((1, block), jnp.float32),
            pltpu.VMEM((1, block), jnp.float32),
            dma, dma, dma, dma((2,)),
            dma((PLANE, secs)), dma((depth // emb,)),
            dma((PLANE - 1, tiles)), dma((PLANE - 1, tiles)), dma,
            dma((planes - 1, tiles)), dma((planes - 1, tiles)),
            dma, dma,
        ],
        compiler_params=pltpu.CompilerParams(collective_id=0, has_side_effects=True, vmem_limit_bytes=VMEM_LIMIT),
        name="whole_step",
    )(ids, pool_len, table, w_first, bias, w_out)


def body(indices, pool_len, tables, w_first, b_first, w_out):
    sec_count = lax.axis_size("section")
    dev_count = lax.axis_size("dev")
    devices = sec_count * dev_count
    dev_rows, n_tables, pool_size = indices.shape
    rows_dev, emb_width = tables.shape
    row_split = devices // n_tables
    position = lax.axis_index("section") * dev_count + lax.axis_index("dev")
    table_id = position // row_split
    first_row = position % row_split * rows_dev
    outgoing = jnp.transpose(indices, (1, 0, 2)).reshape(n_tables, dev_rows * pool_size)
    square = row_split == 1 and sec_count == 2 and dev_count % PLANE == 0
    if square and w_first.shape[0] % emb_width == 0 and dev_rows * pool_size % 128 == 0:
        ids = outgoing.reshape(n_tables, dev_rows * pool_size // 128, 128)
        logits = whole_step(
            sec_count, dev_count, pool_size, ids, pool_len, tables, w_first, b_first[None, :], w_out[None, :]
        )
        return logits.reshape(logits.shape[1])
    outgoing = jnp.repeat(outgoing, row_split, axis=0)
    arrived = lax.all_to_all(outgoing, ("section", "dev"), split_axis=0, concat_axis=0, tiled=True)
    all_rows = devices * dev_rows
    wanted = arrived.reshape(all_rows * pool_size // 128, 128) - first_row
    live_slots = jnp.sum(jnp.where(jnp.arange(n_tables) == table_id, pool_len, 0))
    slot = jnp.arange(128) % pool_size
    usable = (wanted >= 0) & (wanted < rows_dev) & (slot < live_slots)[None, :]
    safe_rows = jnp.where(usable, wanted, rows_dev)
    partial_value = pool_bags(tables, safe_rows, pool_size)
    ordered = jnp.transpose(
        partial_value.reshape(dev_count, sec_count, dev_rows, emb_width), (1, 0, 2, 3)
    )
    received = lax.all_to_all(
        ordered.reshape(devices, dev_rows, emb_width),
        ("section", "dev"),
        split_axis=0,
        concat_axis=0,
        tiled=True,
    )
    summed = jnp.sum(
        received.reshape(n_tables, row_split, dev_rows, emb_width).astype(jnp.float32), axis=1
    )
    features = jnp.transpose(summed.astype(jnp.bfloat16), (1, 0, 2)).reshape(
        dev_rows, n_tables * emb_width
    )
    samples = lax.all_gather(features, "section", axis=0, tiled=True)
    whole_weights = lax.all_gather(w_first, "dev", axis=0, tiled=True)
    pre_act = jnp.dot(samples, whole_weights, preferred_element_type=jnp.float32)
    hidden = jnp.maximum(pre_act + b_first.astype(jnp.float32)[None, :], 0.0)
    logit_part = jnp.sum(hidden * w_out.astype(jnp.float32)[None, :], axis=1)
    return lax.psum(logit_part, "section")


def solution(mesh):
    placed = (
        P(("section", "dev"), None, None),
        P(),
        P(("section", "dev"), None),
        P("dev", "section"),
        P("section"),
        P("section"),
    )
    return jax.shard_map(body, mesh=mesh, in_specs=placed, out_specs=P("dev"), check_vma=False)
```

```python
import functools

import jax
import jax.numpy as jnp
from jax import lax
from jax.experimental import pallas as pl
from jax.experimental.pallas import tpu as pltpu
from jax.sharding import PartitionSpec as P

VMEM_LIMIT = 60 * 1024 * 1024
PLANE = 4
PLANES = 4


def bag_kernel(table_chunks, bags_per_step, pool_size, table_ref, ids_ref, out_ref, staged, wide, sums, sems):
    rows, _ = table_ref.shape
    chunk = rows // table_chunks

    def fetch(c):
        return pltpu.make_async_copy(table_ref.at[pl.ds(c * chunk, chunk)], staged.at[c % 2], sems.at[c % 2])

    fetch(0).start()
    wide[pl.ds(rows, 8), :] = jnp.zeros((8, wide.shape[1]), jnp.float32)
    for c in range(table_chunks):
        if c + 1 < table_chunks:
            fetch(c + 1).start()
        fetch(c).wait()
        step = 256

        def widen(k, carry):
            at = pl.multiple_of(k * step, step)
            wide[pl.ds(c * chunk + at, step), :] = staged[c % 2, pl.ds(at, step), :].astype(jnp.float32)
            return carry

        lax.fori_loop(0, chunk // step, widen, 0)

    def bags(r, carry):
        for b in range(bags_per_step):
            total = None
            for p in range(pool_size):
                row = wide[pl.ds(ids_ref[r, b * pool_size + p], 1), :]
                total = row if total is None else total + row
            sums[pl.ds(r * bags_per_step + b, 1), :] = total
        return carry

    lax.fori_loop(0, ids_ref.shape[0], bags, 0)
    out_ref[...] = sums[...].astype(jnp.bfloat16)


def pool_bags(table, ids, pool_size):
    rows, emb = table.shape
    bags_per_step = ids.shape[1] // pool_size
    n_bags = ids.shape[0] * bags_per_step
    chunks = 8
    return pl.pallas_call(
        functools.partial(bag_kernel, chunks, bags_per_step, pool_size),
        out_shape=jax.ShapeDtypeStruct((n_bags, emb), jnp.bfloat16),
        in_specs=[pl.BlockSpec(memory_space=pl.ANY), pl.BlockSpec(memory_space=pltpu.SMEM)],
        out_specs=pl.BlockSpec(memory_space=pltpu.VMEM),
        scratch_shapes=[
            pltpu.VMEM((2, rows // chunks, emb), jnp.bfloat16),
            pltpu.VMEM((rows + 8, emb), jnp.float32),
            pltpu.VMEM((n_bags, emb), jnp.float32),
            pltpu.SemaphoreType.DMA((2,)),
        ],
        compiler_params=pltpu.CompilerParams(vmem_limit_bytes=VMEM_LIMIT),
        cost_estimate=pl.CostEstimate(flops=n_bags * pool_size * emb * 600, bytes_accessed=rows * emb * 2, transcendentals=0),
        name="pool_bags",
    )(table, ids)


def step_kernel(
    secs, devs, pool_size,
    ids_ref, len_ref, table_ref, w_ref, b_ref, wo_ref, out_ref,
    ids_in, ids_safe, ids_smem, staged, wide, sums, pooled, feats, weights, pre, outgoing, relay, incoming, mine, theirs,
    isend, irecv, icopy, tsem, fsend, frecv, wsend, wrecv, wlocal, psend, precv, lsend, lrecv,
):
    rows, emb = table_ref.shape
    count = secs * devs
    per_dev, hid = w_ref.shape
    depth = PLANE * per_dev
    tables_dev = per_dev // emb
    planes = devs // PLANE
    block = pooled.shape[2]
    tiles = psend.shape[1]
    tile = hid // tiles
    sec, dev = lax.axis_index("section"), lax.axis_index("dev")
    me = sec * devs + dev
    plane, inner = dev // PLANE, lax.rem(dev, PLANE)

    def device(position):
        return {"section": position // devs, "dev": lax.rem(position, devs)}

    chunks = 8
    chunk = rows // chunks

    def fetch(c):
        return pltpu.make_async_copy(table_ref.at[pl.ds(c * chunk, chunk)], staged.at[c % 2], tsem.at[c % 2])

    fetch(0).start()
    own_weights = pltpu.make_async_copy(w_ref, weights.at[inner], wlocal)
    own_weights.start()
    own_ids = pltpu.make_async_copy(ids_ref.at[me], ids_in.at[me], irecv)
    own_ids.start()

    barrier = pltpu.get_barrier_semaphore()
    for k in range(1, count):
        pl.semaphore_signal(barrier, inc=1, device_id=device(lax.rem(me + k, count)))
    pl.semaphore_wait(barrier, count - 1)

    for k in range(1, count):
        other = lax.rem(me + k, count)
        pltpu.make_async_remote_copy(
            src_ref=ids_ref.at[other], dst_ref=ids_in.at[me], send_sem=isend, recv_sem=irecv,
            device_id=device(other),
        ).start()

    shipped = []

    def ship(n):
        cols = pl.ds(n * tile, tile)
        for k in range(1, PLANE):
            copy = pltpu.make_async_remote_copy(
                src_ref=w_ref.at[:, cols], dst_ref=weights.at[inner, :, cols],
                send_sem=wsend.at[k - 1, n], recv_sem=wrecv.at[k - 1, n],
                device_id={"section": sec, "dev": plane * PLANE + lax.rem(inner + k, PLANE)},
            )
            copy.start()
            shipped.append(copy)

    for n in range(tiles // 2):
        ship(n)

    wide[pl.ds(rows, 8), :] = jnp.zeros((8, emb), jnp.float32)
    step = 256
    for c in range(chunks):
        if c + 1 < chunks:
            fetch(c + 1).start()
        fetch(c).wait()

        def widen(k, carry):
            at = pl.multiple_of(k * step, step)
            wide[pl.ds(c * chunk + at, step), :] = staged[c % 2, pl.ds(at, step), :].astype(jnp.float32)
            return carry

        lax.fori_loop(0, chunk // step, widen, 0)

    pltpu.make_async_copy(ids_in, ids_in, irecv).wait()
    lane_slot = lax.rem(lax.broadcasted_iota(jnp.int32, ids_in.shape, 2), pool_size)
    ids_safe[...] = jnp.where(lane_slot < len_ref[me], ids_in[...], rows)
    to_smem = pltpu.make_async_copy(ids_safe, ids_smem, icopy)
    to_smem.start()
    to_smem.wait()

    per_row = 128 // pool_size
    id_rows = ids_in.shape[1]
    block_rows = block // per_row
    owner = me // tables_dev
    to_plane = owner // PLANE
    slot = lax.rem(owner, PLANE) * tables_dev + lax.rem(me, tables_dev)
    column = pl.ds(pl.multiple_of(slot * emb, emb), emb)
    keeps = to_plane == plane
    copies = []
    for k in list(range(1, PLANE)) + [0]:
        to_inner = lax.rem(inner + k, PLANE)

        def bags(n, carry):
            at_plane, r = n // block_rows, lax.rem(n, block_rows)
            line = (at_plane * PLANE + to_inner) * block_rows + r
            source, part = line // id_rows, lax.rem(line, id_rows)
            for q in range(per_row):
                total = None
                for p in range(pool_size):
                    row = wide[pl.ds(ids_smem[source, part, q * pool_size + p], 1), :]
                    total = row if total is None else total + row
                sums[at_plane, to_inner, pl.ds(r * per_row + q, 1), :] = total
            return carry

        lax.fori_loop(0, planes * block_rows, bags, 0)
        pooled[:, to_inner] = sums[:, to_inner].astype(jnp.bfloat16)
        for c in range(secs):
            source_part, dst = pooled.at[:, to_inner], feats.at[:, :, column]
            copy = pltpu.make_async_remote_copy(
                src_ref=source_part, dst_ref=dst,
                send_sem=fsend.at[k, c], recv_sem=frecv.at[slot],
                device_id={"section": lax.rem(sec + c, secs), "dev": to_plane * PLANE + to_inner},
            )
            if k == 0 and c == 0:
                local = pltpu.make_async_copy(source_part, dst, frecv.at[slot])

                @pl.when(keeps)
                def _():
                    local.start()

                @pl.when(jnp.logical_not(keeps))
                def _():
                    copy.start()

                kept = copy
            else:
                copy.start()
                copies.append(copy)
        if k == PLANE - 1:
            for n in range(tiles // 2, 3 * tiles // 4):
                ship(n)
        if k == 0:
            for n in range(3 * tiles // 4, tiles):
                ship(n)
    for t in range(depth // emb):
        part = feats.at[:, :, pl.ds(t * emb, emb)]
        pltpu.make_async_copy(part, part, frecv.at[t]).wait()

    own_weights.wait()
    near = plane + 1 - 2 * lax.rem(plane, 2)
    far = lax.rem(plane + 2, PLANES)
    partials = {}

    def send(src, lane, n, to):
        cols = pl.ds(n * tile, tile)
        copy = pltpu.make_async_remote_copy(
            src_ref=src, dst_ref=incoming.at[lane, :, cols],
            send_sem=psend.at[lane, n], recv_sem=precv.at[lane, n],
            device_id={"section": sec, "dev": to * PLANE + inner},
        )
        copy.start()
        partials[lane, n] = copy

    def pass_on(n):
        cols = pl.ds(n * tile, tile)
        partials[1, n].wait_recv()
        relay[:, cols] = (pre[far, :, cols] + incoming[1, :, cols].astype(jnp.float32)).astype(jnp.bfloat16)
        send(relay.at[:, cols], 2, n, far)

    for n in range(tiles):
        cols = pl.ds(n * tile, tile)
        for k in range(1, PLANE):
            shipped[n * (PLANE - 1) + k - 1].wait_recv()
        got = jnp.dot(
            feats[...].reshape(planes * block, depth), weights[:, :, cols].reshape(depth, tile),
            preferred_element_type=jnp.float32,
        ).reshape(planes, block, tile)
        pre[:, :, cols] = got
        outgoing[:, :, cols] = got.astype(jnp.bfloat16)
        send(outgoing.at[lax.rem(near + 2, PLANES), :, cols], 1, n, near)
        send(outgoing.at[near, :, cols], 0, n, near)
        if n >= 2:
            pass_on(n - 2)
    pass_on(tiles - 2)
    pass_on(tiles - 1)

    acc = jnp.zeros((block, 128), jnp.float32)
    for n in range(tiles):
        cols = pl.ds(n * tile, tile)
        total = pre[plane, :, cols]
        for lane in (0, 2):
            partials[lane, n].wait_recv()
            total = total + incoming[lane, :, cols].astype(jnp.float32)
        hidden = jnp.maximum(total + b_ref[cols].astype(jnp.float32)[None, :], 0.0)
        weighed = hidden * wo_ref[cols].astype(jnp.float32)[None, :]
        for q in range(tile // 128):
            acc = acc + weighed[:, q * 128:(q + 1) * 128]
    mine[...] = jnp.sum(acc.T, axis=0, keepdims=True)
    swap = pltpu.make_async_remote_copy(
        src_ref=mine, dst_ref=theirs, send_sem=lsend, recv_sem=lrecv,
        device_id={"section": 1 - sec, "dev": dev},
    )
    swap.start()
    swap.wait()
    out_ref[...] = mine[...] + theirs[...]
    for copy in list(partials.values()) + shipped + copies:
        copy.wait_send()

    @pl.when(jnp.logical_not(keeps))
    def _():
        kept.wait_send()

    sent = ids_in.at[pl.ds(0, count - 1)]
    pltpu.make_async_copy(sent, sent, isend).wait()


def whole_step(secs, devs, pool_size, ids, pool_len, table, w_first, bias, w_out):
    rows, emb = table.shape
    per_dev, hid = w_first.shape
    count = secs * devs
    planes = devs // PLANE
    depth = PLANE * per_dev
    block = ids.shape[1] * 128 // pool_size * secs
    tiles = 8
    vm = pl.BlockSpec(memory_space=pltpu.VMEM)
    anywhere = pl.BlockSpec(memory_space=pl.ANY)
    dma = pltpu.SemaphoreType.DMA
    return pl.pallas_call(
        functools.partial(step_kernel, secs, devs, pool_size),
        out_shape=jax.ShapeDtypeStruct((1, block), jnp.float32),
        in_specs=[vm, pl.BlockSpec(memory_space=pltpu.SMEM), anywhere, anywhere, vm, vm],
        out_specs=vm,
        scratch_shapes=[
            pltpu.VMEM(ids.shape, jnp.int32),
            pltpu.VMEM(ids.shape, jnp.int32),
            pltpu.SMEM(ids.shape, jnp.int32),
            pltpu.VMEM((2, rows // 8, emb), jnp.bfloat16),
            pltpu.VMEM((rows + 8, emb), jnp.float32),
            pltpu.VMEM((planes, PLANE, block, emb), jnp.float32),
            pltpu.VMEM((planes, PLANE, block, emb), jnp.bfloat16),
            pltpu.VMEM((planes, block, depth), jnp.bfloat16),
            pltpu.VMEM((PLANE, per_dev, hid), jnp.bfloat16),
            pltpu.VMEM((planes, block, hid), jnp.float32),
            pltpu.VMEM((planes, block, hid), jnp.bfloat16),
            pltpu.VMEM((block, hid), jnp.bfloat16),
            pltpu.VMEM((3, block, hid), jnp.bfloat16),
            pltpu.VMEM((1, block), jnp.float32),
            pltpu.VMEM((1, block), jnp.float32),
            dma, dma, dma, dma((2,)),
            dma((PLANE, secs)), dma((depth // emb,)),
            dma((PLANE - 1, tiles)), dma((PLANE - 1, tiles)), dma,
            dma((3, tiles)), dma((3, tiles)),
            dma, dma,
        ],
        compiler_params=pltpu.CompilerParams(collective_id=0, has_side_effects=True, vmem_limit_bytes=VMEM_LIMIT),
        name="whole_step",
    )(ids, pool_len, table, w_first, bias, w_out)


def body(indices, pool_len, tables, w_first, b_first, w_out):
    sec_count = lax.axis_size("section")
    dev_count = lax.axis_size("dev")
    devices = sec_count * dev_count
    dev_rows, n_tables, pool_size = indices.shape
    rows_dev, emb_width = tables.shape
    row_split = devices // n_tables
    position = lax.axis_index("section") * dev_count + lax.axis_index("dev")
    table_id = position // row_split
    first_row = position % row_split * rows_dev
    outgoing = jnp.transpose(indices, (1, 0, 2)).reshape(n_tables, dev_rows * pool_size)
    square = row_split == 1 and sec_count == 2 and dev_count == PLANE * PLANES
    if square and w_first.shape[0] % emb_width == 0 and dev_rows * pool_size % 128 == 0:
        ids = outgoing.reshape(n_tables, dev_rows * pool_size // 128, 128)
        logits = whole_step(
            sec_count, dev_count, pool_size, ids, pool_len, tables, w_first, b_first, w_out
        )
        return logits.reshape(logits.shape[1])
    outgoing = jnp.repeat(outgoing, row_split, axis=0)
    arrived = lax.all_to_all(outgoing, ("section", "dev"), split_axis=0, concat_axis=0, tiled=True)
    all_rows = devices * dev_rows
    wanted = arrived.reshape(all_rows * pool_size // 128, 128) - first_row
    live_slots = jnp.sum(jnp.where(jnp.arange(n_tables) == table_id, pool_len, 0))
    slot = jnp.arange(128) % pool_size
    usable = (wanted >= 0) & (wanted < rows_dev) & (slot < live_slots)[None, :]
    safe_rows = jnp.where(usable, wanted, rows_dev)
    partial_value = pool_bags(tables, safe_rows, pool_size)
    ordered = jnp.transpose(
        partial_value.reshape(dev_count, sec_count, dev_rows, emb_width), (1, 0, 2, 3)
    )
    received = lax.all_to_all(
        ordered.reshape(devices, dev_rows, emb_width),
        ("section", "dev"),
        split_axis=0,
        concat_axis=0,
        tiled=True,
    )
    summed = jnp.sum(
        received.reshape(n_tables, row_split, dev_rows, emb_width).astype(jnp.float32), axis=1
    )
    features = jnp.transpose(summed.astype(jnp.bfloat16), (1, 0, 2)).reshape(
        dev_rows, n_tables * emb_width
    )
    samples = lax.all_gather(features, "section", axis=0, tiled=True)
    whole_weights = lax.all_gather(w_first, "dev", axis=0, tiled=True)
    pre_act = jnp.dot(samples, whole_weights, preferred_element_type=jnp.float32)
    hidden = jnp.maximum(pre_act + b_first.astype(jnp.float32)[None, :], 0.0)
    logit_part = jnp.sum(hidden * w_out.astype(jnp.float32)[None, :], axis=1)
    return lax.psum(logit_part, "section")


def solution(mesh):
    placed = (
        P(("section", "dev"), None, None),
        P(),
        P(("section", "dev"), None),
        P("dev", "section"),
        P("section"),
        P("section"),
    )
    return jax.shard_map(body, mesh=mesh, in_specs=placed, out_specs=P("dev"), check_vma=False)
```
